32 devices in a mesh: dp: 4 (over y, core), head: 2 (over x), kv: 4 (over z).
Axes of the slice: x: 2, y: 2, z: 4, core: 2. Of those that a mesh axis runs over, the one named last changes fastest.
Arguments:
- teacher_query: bfloat16 [4, 1024, 3584], P('dp', 'kv', 'head'), may hold values from -96 to 96
- teacher_key: bfloat16 [4, 1024, 512], P('dp', 'kv', 'head'), may hold values from -8 to 8
- student_query: bfloat16 [4, 1024, 1792], P('dp', 'kv', 'head'), may hold values from -96 to 96
- student_key: bfloat16 [4, 1024, 256], P('dp', 'kv', 'head'), may hold values from -8 to 8
- pair_table: int32 [14, 2], replicated, may hold values from 0 to 27, as said below
Outputs:
- kl: float32 [4, 14, 1024], P('dp', 'head', 'kv')
- head_loss: float32 [14], P('head')
The draws below stay inside these ranges and needn't reach their ends.
Inputs may be any that keep to these rules, and one draw needn't show every extreme that they name: `pair_table`: each of the 28 teacher heads appears exactly once in the table.
All inputs are finite; a program needn't handle non-finite values.
Results may differ from the reference program's by a relative error of at most 0.0003.
Values may be sent and summed in bfloat16 or wider, within the bound.
A program may use at most 64 MiB of HBM per device.

```python
import math
import jax
import jax.numpy as jnp
from jax import lax

HT = 28
KVT = 4
DH = 128
HS = 14
KVS = 2
L = 1024
SEQS = 4


def key_field(key, heads):
    shape = (SEQS, L, heads, DH)
    row_scale = jnp.exp(jax.random.uniform(jax.random.fold_in(key, 1), (SEQS, L, heads, 1), jnp.float32, math.log(0.5), math.log(2.0)))
    base = jnp.clip(jax.random.normal(key, shape, jnp.float32), -4.0, 4.0)
    return base * row_scale


def query_field(key, heads):
    shape = (SEQS, L, heads, DH)
    row_scale = jnp.exp(jax.random.uniform(jax.random.fold_in(key, 1), (SEQS, L, heads, 1), jnp.float32, math.log(0.3), math.log(3.0)))
    return jnp.clip(jax.random.normal(key, shape, jnp.float32), -5.0, 5.0) * row_scale


def draw_teacher_key(key, part):
    keys = key_field(jax.random.fold_in(key, 11), KVT)
    return keys.reshape(SEQS, L, KVT * DH).astype(jnp.bfloat16)


def draw_student_key(key, part):
    keys = key_field(jax.random.fold_in(key, 12), KVS)
    return keys.reshape(SEQS, L, KVS * DH).astype(jnp.bfloat16)


def draw_teacher_query(key, part):
    queries = query_field(jax.random.fold_in(key, 13), HT)
    return queries.reshape(SEQS, L, HT * DH).astype(jnp.bfloat16)


def draw_student_query(key, part):
    queries = query_field(jax.random.fold_in(key, 14), HS)
    return queries.reshape(SEQS, L, HS * DH).astype(jnp.bfloat16)


def draw_pair_table(key, part):
    order = jax.random.permutation(jax.random.fold_in(key, 15), HT)
    return order.astype(jnp.int32).reshape(HS, 2)


def setup_inputs(seed: int = 0) -> dict:
    streams_of = jax.random.split(jax.random.key(seed), 6)
    teacher_query = draw_teacher_query(jax.random.fold_in(streams_of[5], 71), 0)
    teacher_key = draw_teacher_key(jax.random.fold_in(streams_of[5], 71), 0)
    student_query = draw_student_query(jax.random.fold_in(streams_of[5], 71), 0)
    student_key = draw_student_key(jax.random.fold_in(streams_of[5], 71), 0)
    pair_table = draw_pair_table(jax.random.fold_in(streams_of[5], 71), 0)
    return dict(teacher_query=teacher_query, teacher_key=teacher_key, student_query=student_query, student_key=student_key, pair_table=pair_table)


masked_value = -1e+30

def masked_logits(query_rows, key_rows, causal_mask):
    scale = 1.0 / math.sqrt(DH)
    product = jnp.dot(query_rows.astype(jnp.float32), key_rows.astype(jnp.float32).T, precision=lax.Precision.HIGHEST, preferred_element_type=jnp.float32) * scale
    return jnp.where(causal_mask, product, masked_value)

def log_total(logits, causal_mask):
    row_max = lax.optimization_barrier(jnp.max(logits, axis=-1))
    weights = jnp.where(causal_mask, jnp.exp(logits - row_max[:, None]), 0.0)
    return row_max + jnp.log(lax.optimization_barrier(jnp.sum(weights, axis=-1)))

def reference(teacher_query, teacher_key, student_query, student_key, pair_table):
    teacher_q = teacher_query.reshape(SEQS, L, HT, DH)
    teacher_k = teacher_key.reshape(SEQS, L, KVT, DH)
    student_q = student_query.reshape(SEQS, L, HS, DH)
    student_k = student_key.reshape(SEQS, L, KVS, DH)
    group_teacher = HT // KVT
    group_student = HS // KVS
    positions = jnp.arange(L, dtype=jnp.int32)
    causal_mask = positions[None, :] <= positions[:, None]

    def one_item(flat_index):
        sequence = flat_index // HS
        student = flat_index % HS
        s_logits = masked_logits(student_q[sequence, :, student], student_k[sequence, :, student // group_student], causal_mask)
        s_lse = log_total(s_logits, causal_mask)
        total = jnp.zeros((L,), jnp.float32)
        for column in range(2):
            teacher = pair_table[student, column]
            t_logits = masked_logits(teacher_q[sequence, :, teacher], teacher_k[sequence, :, teacher // group_teacher], causal_mask)
            t_lse = log_total(t_logits, causal_mask)
            probs = jnp.where(causal_mask, jnp.exp(t_logits - t_lse[:, None]), 0.0)
            total = total + (lax.optimization_barrier(jnp.sum(probs * (t_logits - s_logits), axis=-1)) - t_lse + s_lse)
        return total
    kl = lax.map(one_item, jnp.arange(SEQS * HS, dtype=jnp.int32)).reshape(SEQS, HS, L)
    head_loss = lax.optimization_barrier(jnp.sum(kl, axis=(0, 2))) / (SEQS * L)
    return (kl, head_loss)
```

```python
import functools
import math

import jax
import jax.numpy as jnp
from jax import lax
from jax.experimental import pallas as pl
from jax.experimental.pallas import tpu as pltpu
from jax.sharding import PartitionSpec as P

HT = 28
KVT = 4
DH = 128
HS = 14
KVS = 2

MESH = pl.DeviceIdType.MESH
LOWEST = -1e30


def nn(a, b):
    return jnp.dot(a, b, preferred_element_type=jnp.float32)


def flip(x):
    n = x.shape[1]
    eye = (
        lax.broadcasted_iota(jnp.int32, (n, n), 0) == lax.broadcasted_iota(jnp.int32, (n, n), 1)
    ).astype(jnp.bfloat16)
    out = lax.dot_general(eye, x, (((1,), (1,)), ((), ())), preferred_element_type=jnp.float32)
    return out.astype(jnp.bfloat16)


def kernel(
    n_dp, n_head, n_kv, rows,
    table, tq_hbm, tk_hbm, sq_hbm, sk_hbm,
    kl_ref, loss_ref,
    tq, tk, sq, sk,
    tq_t, sq_t, key_t, mixed, t_max, s_max, s_sum,
    inverse, acc, acc_in, sums,
    load_sem, x_send, x_recv, z_send, z_recv, sum_send, sum_recv,
):
    n_t, n_s = HT // n_head, HS // n_head
    g_t, g_s = KVT // n_head, KVS // n_head
    per_t, per_s = HT // KVT, HS // KVS
    dp, hd, kv = lax.axis_index("dp"), lax.axis_index("head"), lax.axis_index("kv")
    n_rank = n_dp * n_kv
    rank = dp * n_kv + kv
    scale = 1.0 / math.sqrt(DH)
    rate = scale * math.log2(math.e)

    loads = [
        pltpu.make_async_copy(sk_hbm.at[0], sk.at[hd, kv], load_sem.at[0]),
        pltpu.make_async_copy(tk_hbm.at[0], tk.at[kv], load_sem.at[1]),
        pltpu.make_async_copy(sq_hbm.at[0], sq.at[hd], load_sem.at[2]),
        pltpu.make_async_copy(tq_hbm.at[0], tq, load_sem.at[3]),
    ]
    for load in loads:
        load.start()

    barrier = pltpu.get_barrier_semaphore()

    def greet(peer, carry):
        @pl.when(peer != rank)
        def _():
            pl.semaphore_signal(
                barrier, inc=1, device_id={"dp": peer // n_kv, "kv": peer % n_kv},
                device_id_type=MESH,
            )
        return carry

    for step in range(1, n_head):
        pl.semaphore_signal(
            barrier, inc=1, device_id={"head": (hd + step) % n_head}, device_id_type=MESH
        )
    lax.fori_loop(0, n_rank, greet, 0)

    entries = [table[k // 2, k % 2] for k in range(HT)]
    for t in range(n_t):
        found = jnp.int32(0)
        for k in range(HT):
            found = jnp.where(entries[k] == hd * n_t + t, k // 2, found)
        inverse[t] = found

    for load in loads:
        load.wait()
    pl.semaphore_wait(barrier, n_rank - 1 + n_head - 1)

    def across(slot, step, src, dst):
        return pltpu.make_async_remote_copy(
            src_ref=src, dst_ref=dst, send_sem=x_send.at[slot, step - 1],
            recv_sem=x_recv.at[slot, step - 1],
            device_id={"head": (hd + step) % n_head}, device_id_type=MESH,
        )

    def upward(block, piece):
        ref = tk.at[block] if piece is n_head else sk.at[piece, block]
        return pltpu.make_async_remote_copy(
            src_ref=ref, dst_ref=ref, send_sem=z_send.at[block, piece],
            recv_sem=z_recv.at[block, piece],
            device_id={"kv": jnp.minimum(kv + 1, n_kv - 1)}, device_id_type=MESH,
        )

    pieces = [n_head] + [(hd + s) % n_head for s in range(n_head)]
    not_last = kv < n_kv - 1

    keys_over = [across(0, s, sk.at[hd, kv], sk.at[hd, kv]) for s in range(1, n_head)]
    queries_over = [across(1, s, sq.at[hd], sq.at[hd]) for s in range(1, n_head)]
    for copy in keys_over:
        copy.start()

    @pl.when(not_last)
    def _():
        upward(kv, n_head).start()
        upward(kv, hd).start()

    for copy in queries_over:
        copy.start()

    for h in range(n_t):
        tq_t[h] = flip(tq[:, h * DH:(h + 1) * DH])
    for h in range(n_s):
        sq_t[hd * n_s + h] = flip(sq[hd, :, h * DH:(h + 1) * DH])

    key_t[:, 2 * DH:] = jnp.ones((g_t * KVS, 16, rows), jnp.bfloat16)
    for copy in keys_over:
        copy.wait()

    @pl.when(not_last)
    def _():
        for s in range(1, n_head):
            upward(kv, (hd + s) % n_head).start()

    visible = lax.broadcasted_iota(jnp.int32, (rows, rows), 0) <= lax.broadcasted_iota(
        jnp.int32, (rows, rows), 1
    )

    def fold(block, diagonal):
        for g in range(g_t):
            flipped = flip(tk[block, :, g * DH:(g + 1) * DH])
            for j in range(KVS):
                key_t[g * KVS + j, :DH] = flipped
        for j in range(KVS):
            flipped = flip(sk[j // g_s, block, :, j % g_s * DH:(j % g_s + 1) * DH])
            for g in range(g_t):
                key_t[g * KVS + j, DH:2 * DH] = flipped

        def weigh(logits, high, row):
            if diagonal:
                logits = jnp.where(visible, logits, LOWEST)
            top = jnp.max(logits, axis=0, keepdims=True)
            if diagonal:
                decay = None
            else:
                old = high[row]
                top = jnp.maximum(old, top)
                decay = jnp.exp2((old - top) * rate)
            weights = jnp.exp2((logits - top) * rate)
            high[row] = top
            return weights, decay

        for h in range(n_t):
            g = h // per_t
            logits = nn(tk[block, :, g * DH:(g + 1) * DH], tq_t[h])
            weights, decay = weigh(logits, t_max, h)
            part = nn(key_t[g * KVS + inverse[h] // per_s], weights.astype(jnp.bfloat16))
            mixed[h] = part if diagonal else mixed[h] * decay + part
        for h in range(n_s):
            g = h // per_s
            logits = nn(sk[hd, block, :, g * DH:(g + 1) * DH], sq_t[hd * n_s + h])
            weights, decay = weigh(logits, s_max, h)
            part = jnp.sum(weights, axis=0, keepdims=True)
            s_sum[h] = part if diagonal else s_sum[h] * decay + part

    fold(kv, True)

    def step(s, carry):
        block = kv - s
        for piece in pieces:
            upward(block, piece).wait_recv()

            @pl.when(not_last)
            def _():
                upward(block, piece).start()
        fold(block, False)
        return carry

    lax.fori_loop(1, kv + 1, step, 0)

    for copy in queries_over:
        copy.wait()
    for s in range(1, n_head):
        d = (hd + s) % n_head
        for h in range(n_s):
            sq_t[d * n_s + h] = flip(sq[d, :, h * DH:(h + 1) * DH])

    pad = acc.shape[0] // n_head
    place = lax.broadcasted_iota(jnp.int32, acc.shape, 0)
    total = jnp.zeros(acc.shape, jnp.float32)
    for h in range(n_t):
        partner = inverse[h]
        own = mixed[h, :DH] * tq_t[h].astype(jnp.float32)
        other = mixed[h, DH:2 * DH] * sq_t[partner].astype(jnp.float32)
        mass = mixed[h, 2 * DH:2 * DH + 1]
        value = jnp.sum(own - other, axis=0, keepdims=True) * scale / mass
        value = value - (t_max[h] * scale + jnp.log(mass))
        row = (partner // n_s) * pad + partner % n_s
        total = total + jnp.where(place == row, value, 0.0)
    acc[...] = total

    returns = [
        across(2, s, acc.at[pl.ds(((hd + s) % n_head) * pad, pad)], acc_in.at[s - 1])
        for s in range(1, n_head)
    ]
    for copy in returns:
        copy.start()
    lse = jnp.concatenate(
        [s_max[h] * scale + jnp.log(s_sum[h]) for h in range(n_s)]
        + [jnp.zeros((1, rows), jnp.float32)] * (pad - n_s),
        axis=0,
    )
    kl = acc[pl.ds(hd * pad, pad)] + 2.0 * lse
    for s in range(1, n_head):
        returns[s - 1].wait()
        kl = kl + acc_in[s - 1]
    kl_ref[0] = kl[:n_s]
    sums[rank] = jnp.broadcast_to(jnp.sum(kl, axis=1, keepdims=True), (pad, 128))

    def share(peer, place):
        return pltpu.make_async_remote_copy(
            src_ref=sums.at[rank], dst_ref=sums.at[rank],
            send_sem=sum_send.at[peer], recv_sem=sum_recv.at[place],
            device_id={"dp": peer // n_kv, "kv": peer % n_kv}, device_id_type=MESH,
        )

    def send(peer, carry):
        @pl.when(peer != rank)
        def _():
            share(peer, rank).start()
        return carry

    def land(peer, carry):
        @pl.when(peer != rank)
        def _():
            share(peer, rank).wait_send()
            share(peer, peer).wait_recv()
        return carry

    lax.fori_loop(0, n_rank, send, 0)

    @pl.when(not_last)
    def _():
        def drain(block, carry):
            for piece in pieces:
                upward(block, piece).wait_send()
            return carry
        lax.fori_loop(0, kv + 1, drain, 0)

    lax.fori_loop(0, n_rank, land, 0)
    whole = jnp.sum(sums[...], axis=0)
    diagonal = lax.broadcasted_iota(jnp.int32, whole.shape, 0) == lax.broadcasted_iota(
        jnp.int32, whole.shape, 1
    )
    line = jnp.sum(jnp.where(diagonal, whole, 0.0), axis=0, keepdims=True)
    loss_ref[...] = line[:, :n_s] / (n_dp * rows * n_kv)


def per_device(teacher_query, teacher_key, student_query, student_key, pair_table):
    n_dp, n_head, n_kv = lax.axis_size("dp"), lax.axis_size("head"), lax.axis_size("kv")
    seq_dev, rows, wide_t = teacher_query.shape
    assert seq_dev == 1
    n_t, n_s = HT // n_head, HS // n_head
    g_t, g_s = KVT // n_head, KVS // n_head
    n_rank = n_dp * n_kv
    pad = -(-n_s // 8) * 8
    f32, bf16 = jnp.float32, jnp.bfloat16
    dma = pltpu.SemaphoreType.DMA
    kl, loss = pl.pallas_call(
        functools.partial(kernel, n_dp, n_head, n_kv, rows),
        out_shape=(
            jax.ShapeDtypeStruct((1, n_s, rows), f32),
            jax.ShapeDtypeStruct((1, n_s), f32),
        ),
        in_specs=[pl.BlockSpec(memory_space=pltpu.SMEM)]
        + [pl.BlockSpec(memory_space=pl.ANY)] * 4,
        out_specs=(
            pl.BlockSpec(memory_space=pltpu.VMEM),
            pl.BlockSpec(memory_space=pltpu.VMEM),
        ),
        scratch_shapes=[
            pltpu.VMEM((rows, wide_t), bf16),
            pltpu.VMEM((n_kv, rows, g_t * DH), bf16),
            pltpu.VMEM((n_head, rows, n_s * DH), bf16),
            pltpu.VMEM((n_head, n_kv, rows, g_s * DH), bf16),
            pltpu.VMEM((n_t, DH, rows), bf16),
            pltpu.VMEM((HS, DH, rows), bf16),
            pltpu.VMEM((g_t * KVS, 2 * DH + 16, rows), bf16),
            pltpu.VMEM((n_t, 2 * DH + 16, rows), f32),
            pltpu.VMEM((n_t, 1, rows), f32),
            pltpu.VMEM((n_s, 1, rows), f32),
            pltpu.VMEM((n_s, 1, rows), f32),
            pltpu.SMEM((n_t,), jnp.int32),
            pltpu.VMEM((n_head * pad, rows), f32),
            pltpu.VMEM((max(n_head - 1, 1), pad, rows), f32),
            pltpu.VMEM((n_rank, pad, 128), f32),
            dma((4,)),
            dma((3, max(n_head - 1, 1))),
            dma((3, max(n_head - 1, 1))),
            dma((n_kv, n_head + 1)),
            dma((n_kv, n_head + 1)),
            dma((n_rank,)),
            dma((n_rank,)),
        ],
        compiler_params=pltpu.CompilerParams(collective_id=0, has_side_effects=True),
    )(pair_table, teacher_query, teacher_key, student_query, student_key)
    return kl, loss.reshape(n_s)


def solution(mesh):
    split = P("dp", "kv", "head")
    return jax.shard_map(
        per_device,
        mesh=mesh,
        in_specs=(split, split, split, split, P()),
        out_specs=(P("dp", "head", "kv"), P("head")),
        check_vma=False,
    )
```

```python
import functools
import math

import jax
import jax.numpy as jnp
from jax import lax
from jax.experimental import pallas as pl
from jax.experimental.pallas import tpu as pltpu
from jax.sharding import PartitionSpec as P

HT = 28
KVT = 4
DH = 128
HS = 14
KVS = 2

MESH = pl.DeviceIdType.MESH
LOWEST = -1e30


def nn(a, b):
    return jnp.dot(a, b, preferred_element_type=jnp.float32)


def flip(x):
    n = x.shape[1]
    eye = (
        lax.broadcasted_iota(jnp.int32, (n, n), 0) == lax.broadcasted_iota(jnp.int32, (n, n), 1)
    ).astype(jnp.bfloat16)
    out = lax.dot_general(eye, x, (((1,), (1,)), ((), ())), preferred_element_type=jnp.float32)
    return out.astype(jnp.bfloat16)


def kernel(
    n_dp, n_head, n_kv, rows,
    table, tq_hbm, tk_hbm, sq_hbm, sk_hbm,
    kl_ref, loss_ref,
    tq, tk, sq, sk,
    tq_t, sq_t, key_t, mixed, t_max, s_max, s_sum,
    inverse, acc, acc_in, sums_out, sums,
    load_sem, x_send, x_recv, z_send, z_recv, sum_send, sum_recv,
):
    n_t, n_s = HT // n_head, HS // n_head
    g_t, g_s = KVT // n_head, KVS // n_head
    per_t, per_s = HT // KVT, HS // KVS
    dp, hd, kv = lax.axis_index("dp"), lax.axis_index("head"), lax.axis_index("kv")
    n_rank = n_dp * n_head * n_kv
    rank = (dp * n_head + hd) * n_kv + kv
    scale = 1.0 / math.sqrt(DH)
    rate = scale * math.log2(math.e)

    loads = [
        pltpu.make_async_copy(sk_hbm.at[0], sk.at[hd, kv], load_sem.at[0]),
        pltpu.make_async_copy(tk_hbm.at[0], tk.at[kv], load_sem.at[1]),
        pltpu.make_async_copy(sq_hbm.at[0], sq.at[hd], load_sem.at[2]),
        pltpu.make_async_copy(tq_hbm.at[0], tq, load_sem.at[3]),
    ]
    for load in loads:
        load.start()

    barrier = pltpu.get_barrier_semaphore()

    def coordinates(peer):
        return (peer // (n_head * n_kv), peer // n_kv % n_head, peer % n_kv)

    def greet(peer, carry):
        @pl.when(peer != rank)
        def _():
            pl.semaphore_signal(
                barrier, inc=1, device_id=coordinates(peer), device_id_type=MESH
            )
        return carry

    lax.fori_loop(0, n_rank, greet, 0)

    entries = [table[k % 2, k // 2] for k in range(HT)]
    for t in range(n_t):
        found = jnp.int32(0)
        for k in range(HT):
            found = jnp.where(entries[k] == hd * n_t + t, k // 2, found)
        inverse[t] = found

    for load in loads:
        load.wait()
    pl.semaphore_wait(barrier, n_rank - 1)

    def across(slot, step, src, dst):
        return pltpu.make_async_remote_copy(
            src_ref=src, dst_ref=dst, send_sem=x_send.at[slot, step - 1],
            recv_sem=x_recv.at[slot, step - 1],
            device_id={"head": (hd + step) % n_head}, device_id_type=MESH,
        )

    def upward(block, piece):
        ref = tk.at[block] if piece is n_head else sk.at[piece, block]
        return pltpu.make_async_remote_copy(
            src_ref=ref, dst_ref=ref, send_sem=z_send.at[block, piece],
            recv_sem=z_recv.at[block, piece],
            device_id={"kv": jnp.minimum(kv + 1, n_kv - 1)}, device_id_type=MESH,
        )

    def launch(piece):
        @pl.when(not_last)
        def _():
            upward(kv, piece).start()

    pieces = [n_head] + [(hd + s) % n_head for s in range(n_head)]
    not_last = kv < n_kv - 1

    keys_over = [across(0, s, sk.at[hd, kv], sk.at[hd, kv]) for s in range(1, n_head)]
    queries_over = [across(1, s, sq.at[hd], sq.at[hd]) for s in range(1, n_head)]
    for copy in keys_over:
        copy.start()

    launch(n_head)
    launch(hd)

    for copy in queries_over:
        copy.start()

    for h in range(n_t):
        tq_t[h] = flip(tq[:, h * DH:(h + 1) * DH])
    for h in range(n_s):
        sq_t[hd * n_s + h] = flip(sq[hd, :, h * DH:(h + 1) * DH])

    key_t[:, 2 * DH:] = jnp.ones((g_t * KVS, 16, rows), jnp.bfloat16)
    for copy in keys_over:
        copy.wait()

    for s in range(1, n_head):
        launch((hd + s) % n_head)

    visible = lax.broadcasted_iota(jnp.int32, (rows, rows), 0) <= lax.broadcasted_iota(
        jnp.int32, (rows, rows), 1
    )

    def fold(block, diagonal):
        for g in range(g_t):
            flipped = flip(tk[block, :, g * DH:(g + 1) * DH])
            for j in range(KVS):
                key_t[g * KVS + j, :DH] = flipped
        for j in range(KVS):
            flipped = flip(sk[j // g_s, block, :, j % g_s * DH:(j % g_s + 1) * DH])
            for g in range(g_t):
                key_t[g * KVS + j, DH:2 * DH] = flipped

        def weigh(logits, high, row):
            if diagonal:
                logits = jnp.where(visible, logits, LOWEST)
            top = jnp.max(logits, axis=0, keepdims=True)
            if diagonal:
                decay = None
            else:
                old = high[row]
                top = jnp.maximum(old, top)
                decay = jnp.exp2((old - top) * rate)
            weights = jnp.exp2((logits - top) * rate)
            high[row] = top
            return weights, decay

        for h in range(n_t):
            g = h // per_t
            logits = nn(tk[block, :, g * DH:(g + 1) * DH], tq_t[h])
            weights, decay = weigh(logits, t_max, h)
            part = nn(key_t[g * KVS + inverse[h] // per_s], weights.astype(jnp.bfloat16))
            mixed[h] = part if diagonal else mixed[h] * decay + part
        for h in range(n_s):
            g = h // per_s
            logits = nn(sk[hd, block, :, g * DH:(g + 1) * DH], sq_t[hd * n_s + h])
            weights, decay = weigh(logits, s_max, h)
            part = jnp.sum(weights, axis=0, keepdims=True)
            s_sum[h] = part if diagonal else s_sum[h] * decay + part

    fold(kv, True)

    def step(s, carry):
        block = kv - s
        for piece in pieces:
            upward(block, piece).wait_recv()

            @pl.when(not_last)
            def _():
                upward(block, piece).start()
        fold(block, False)
        return carry

    lax.fori_loop(1, kv + 1, step, 0)

    for copy in queries_over:
        copy.wait()
    for s in range(1, n_head):
        d = (hd + s) % n_head
        for h in range(n_s):
            sq_t[d * n_s + h] = flip(sq[d, :, h * DH:(h + 1) * DH])

    pad = acc.shape[0] // n_head
    place = lax.broadcasted_iota(jnp.int32, acc.shape, 0)
    total = jnp.zeros(acc.shape, jnp.float32)
    for h in range(n_t):
        partner = inverse[h]
        own = mixed[h, :DH] * tq_t[h].astype(jnp.float32)
        other = mixed[h, DH:2 * DH] * sq_t[partner].astype(jnp.float32)
        mass = mixed[h, 2 * DH:2 * DH + 1]
        value = jnp.sum(own - other, axis=0, keepdims=True) * scale / mass
        value = value - (t_max[h] * scale + jnp.log(mass))
        row = (partner // n_s) * pad + partner % n_s
        total = total + jnp.where(place == row, value, 0.0)
    acc[...] = total

    returns = [
        across(2, s, acc.at[pl.ds(((hd + s) % n_head) * pad, pad)], acc_in.at[s - 1])
        for s in range(1, n_head)
    ]
    for copy in returns:
        copy.start()
    lse = jnp.concatenate(
        [s_max[h] * scale + jnp.log(s_sum[h]) for h in range(n_s)]
        + [jnp.zeros((1, rows), jnp.float32)] * (pad - n_s),
        axis=0,
    )
    mine = jnp.where(place // pad == hd, 2.0 * jnp.concatenate([lse] * n_head, axis=0), 0.0)
    column = jnp.sum(total + mine, axis=1, keepdims=True)
    across_lanes = lax.broadcasted_iota(jnp.int32, (n_head * pad, 128), 1)
    down_rows = lax.broadcasted_iota(jnp.int32, (n_head * pad, 128), 0)
    for d in range(n_head):
        sums_out[d] = jnp.sum(
            jnp.where(down_rows == across_lanes + d * pad, column, 0.0), axis=0, keepdims=True
        )

    def share(peer, place):
        return pltpu.make_async_remote_copy(
            src_ref=sums_out.at[peer // n_kv % n_head], dst_ref=sums.at[rank],
            send_sem=sum_send.at[peer], recv_sem=sum_recv.at[place],
            device_id=coordinates(peer), device_id_type=MESH,
        )

    def send(peer, carry):
        @pl.when(peer != rank)
        def _():
            share(peer, rank).start()
        return carry

    def land(peer, carry):
        @pl.when(peer != rank)
        def _():
            share(peer, rank).wait_send()
            share(peer, peer).wait_recv()
        return carry

    lax.fori_loop(0, n_rank, send, 0)
    sums[rank] = sums_out[hd]
    kl = acc[pl.ds(hd * pad, pad)] + 2.0 * lse
    for s in range(1, n_head):
        returns[s - 1].wait()
        kl = kl + acc_in[s - 1]
    for h in range(n_s):
        kl_ref[h] = kl[h:h + 1]

    @pl.when(not_last)
    def _():
        def drain(block, carry):
            for piece in pieces:
                upward(block, piece).wait_send()
            return carry
        lax.fori_loop(0, kv + 1, drain, 0)

    lax.fori_loop(0, n_rank, land, 0)
    line = jnp.sum(sums[...], axis=0)
    loss_ref[...] = line[:, :n_s] / (n_dp * rows * n_kv)


def finish(kl_in, loss_in, kl_ref, loss_ref):
    kl_ref[...] = kl_in[...]
    loss_ref[...] = loss_in[...]


def per_device(teacher_query, teacher_key, student_query, student_key, pair_table):
    n_dp, n_head, n_kv = lax.axis_size("dp"), lax.axis_size("head"), lax.axis_size("kv")
    seq_dev, rows, wide_t = teacher_query.shape
    assert seq_dev == 1
    n_t, n_s = HT // n_head, HS // n_head
    g_t, g_s = KVT // n_head, KVS // n_head
    n_rank = n_dp * n_head * n_kv
    pad = -(-n_s // 8) * 8
    f32, bf16 = jnp.float32, jnp.bfloat16
    dma = pltpu.SemaphoreType.DMA
    kl, loss = pl.pallas_call(
        functools.partial(kernel, n_dp, n_head, n_kv, rows),
        out_shape=(
            jax.ShapeDtypeStruct((n_s, 1, rows), f32),
            jax.ShapeDtypeStruct((1, n_s), f32),
        ),
        in_specs=[pl.BlockSpec(memory_space=pltpu.SMEM)]
        + [pl.BlockSpec(memory_space=pl.ANY)] * 4,
        out_specs=(
            pl.BlockSpec(memory_space=pltpu.VMEM),
            pl.BlockSpec(memory_space=pltpu.VMEM),
        ),
        scratch_shapes=[
            pltpu.VMEM((rows, wide_t), bf16),
            pltpu.VMEM((n_kv, rows, g_t * DH), bf16),
            pltpu.VMEM((n_head, rows, n_s * DH), bf16),
            pltpu.VMEM((n_head, n_kv, rows, g_s * DH), bf16),
            pltpu.VMEM((n_t, DH, rows), bf16),
            pltpu.VMEM((HS, DH, rows), bf16),
            pltpu.VMEM((g_t * KVS, 2 * DH + 16, rows), bf16),
            pltpu.VMEM((n_t, 2 * DH + 16, rows), f32),
            pltpu.VMEM((n_t, 1, rows), f32),
            pltpu.VMEM((n_s, 1, rows), f32),
            pltpu.VMEM((n_s, 1, rows), f32),
            pltpu.SMEM((n_t,), jnp.int32),
            pltpu.VMEM((n_head * pad, rows), f32),
            pltpu.VMEM((max(n_head - 1, 1), pad, rows), f32),
            pltpu.VMEM((n_head, 1, 128), f32),
            pltpu.VMEM((n_rank, 1, 128), f32),
            dma((4,)),
            dma((3, max(n_head - 1, 1))),
            dma((3, max(n_head - 1, 1))),
            dma((n_kv, n_head + 1)),
            dma((n_kv, n_head + 1)),
            dma((n_rank,)),
            dma((n_rank,)),
        ],
        compiler_params=pltpu.CompilerParams(collective_id=0, has_side_effects=True),
    )(pair_table.T, teacher_query, teacher_key, student_query, student_key)
    kl, loss = pl.pallas_call(
        finish,
        out_shape=(
            jax.ShapeDtypeStruct((n_s, 1, rows), f32),
            jax.ShapeDtypeStruct((1, n_s), f32),
        ),
        in_specs=[pl.BlockSpec(memory_space=pltpu.VMEM)] * 2,
        out_specs=(
            pl.BlockSpec(memory_space=pltpu.VMEM),
            pl.BlockSpec(memory_space=pltpu.VMEM),
        ),
    )(kl, loss)
    return kl.reshape(1, n_s, rows), loss.reshape(n_s)


def solution(mesh):
    split = P("dp", "kv", "head")
    return jax.shard_map(
        per_device,
        mesh=mesh,
        in_specs=(split, split, split, split, P()),
        out_specs=(P("dp", "head", "kv"), P("head")),
        check_vma=False,
    )
```
